32 devices in a mesh: section: 2 (over y), dp: 16 (over z, x, core).
Axes of the slice: x: 2, y: 2, z: 4, core: 2. Of those that a mesh axis runs over, the one named last changes fastest.
Arguments:
- tokens: bfloat16 [4, 512, 2048], P(None, 'dp'), may hold values from -6 to 6
- norm_gain: bfloat16 [2, 2048], P('section'), may hold values from 0.25 to 1.75
- router_weight: bfloat16 [2, 2048, 16], P('section'), may hold values from -0.125 to 0.125
- gate_weight: bfloat16 [2, 16, 2048, 768], P('section', 'dp'), may hold values from -0.125 to 0.125
- up_weight: bfloat16 [2, 16, 2048, 768], P('section', 'dp'), may hold values from -0.125 to 0.125
- down_weight: bfloat16 [2, 16, 768, 2048], P('section', 'dp'), may hold values from -0.21875 to 0.21875
- routing: int32 [2, 4, 512, 6], P('section', None, 'dp'), may hold values from 0 to 15, all different within a row; in each aligned block of 32 rows (0 to 31, 32 to 63, ..., all dimensions but the last counted through in order) at most 13 rows name the same one
Outputs:
- layer_outputs: bfloat16 [2, 4, 512, 2048], P('section', None, 'dp')
- router_grad: float32 [2, 2048, 16], P('section', 'dp')
The draws below stay inside these ranges and needn't reach their ends.
Inputs may be any that keep to these rules, and one draw needn't show every extreme that they name: `routing`: each token names 6 different experts. Among one index of dp's 32 tokens of one micro-batch and layer, at most 13 name the same expert, and in some of these blocks exactly 13 do.
All inputs are finite; a program needn't handle non-finite values.
Results may differ from the reference program's by a relative error of at most 0.019.
Values may be sent and summed in bfloat16 or wider, within the bound.
No kernel may reach another device: no remote copies, remote signals or barrier semaphores. Data moves between devices by JAX's collectives and lax.ppermute only.
A program may use at most 64 MiB of HBM per device.

```python
import math
import jax
import jax.numpy as jnp
import numpy as np
from jax import lax

D = 2048
FFE = 768
TOPK = 6
MICRO = 4
MB_TOK = 32
EXPERTS = 16
TOKENS = 512
CAP = 13
N_SECTION = 2
N_DP = 16


def raised(values, stream_key, source, target, shards_of, factor):
    def block_of(position):
        return (jnp.arange(values.shape[position]) // (values.shape[position] // shards_of)).reshape((-1,) + (1,) * (values.ndim - 1 - position))

    first = jax.random.permutation(stream_key, shards_of)[block_of(target)]
    other_side = (block_of(target) + shards_of // 2) % shards_of
    return jnp.where((block_of(source) == first) | (block_of(source) == other_side), factor * values, values)


def block_scale(rng, dims, cuts, smallest, high):
    factor_of = 1.0
    for dim, parts in cuts:
        heights = jax.random.uniform(jax.random.fold_in(jax.random.fold_in(rng, 6), dim), (parts,), jnp.float32, smallest / len(cuts), high / len(cuts))
        factor_of = factor_of * jnp.repeat(jnp.exp(heights), dims[dim] // parts).reshape((-1,) + (1,) * (len(dims) - 1 - dim))
    return factor_of


def deal_out(rng, own, number, rows, amount, top, most, lean):
    sequence = jax.random.permutation(rng, amount)
    crowded, common = portions_of(amount, rows * top, most, lean, True), portions_of(amount, rows * top, most, lean, False)
    places = jnp.arange(amount)

    def named(lengths, offset_by):
        used = int((lengths > 0).sum())
        fixed = max(1, used // 4)
        moved = fixed + (places - fixed + offset_by * (used - fixed)) % max(1, amount - fixed)
        return jnp.zeros((amount,), jnp.int32).at[sequence[jnp.where(places < fixed, places, moved)]].set(jnp.asarray(lengths, jnp.int32))

    lengths = jnp.where(number % 4 == 0, named(crowded, number // 4), named(common, number - number // 4 - 1))
    mixed = jax.random.permutation(jax.random.fold_in(own, 3), amount)
    source_of, receiver = mixed[0:amount // 2 * 2:2], mixed[1:amount // 2 * 2:2]
    slack = jnp.minimum(lengths[source_of] - 1, most - lengths[receiver]) // 2
    slack = jnp.where((source_of == sequence[0]) | (receiver == sequence[0]) | (lengths[receiver] == 0), 0, jnp.maximum(slack, 0))
    moved = jax.random.randint(jax.random.fold_in(own, 4), (amount // 2,), 0, 1 << 20) % (slack + 1)
    lengths = lengths.at[source_of].add(-moved).at[receiver].add(moved)
    items = jnp.searchsorted(jnp.cumsum(lengths), jnp.arange(rows * top), side="right").astype(jnp.int32)
    listing = items.reshape(top, rows).T
    listing = listing[jax.random.permutation(jax.random.fold_in(own, 1), rows)]
    offset_by = jax.random.randint(jax.random.fold_in(own, 2), (rows, 1), 0, top)
    return jnp.take_along_axis(listing, (jnp.arange(top)[None, :] + offset_by) % top, axis=1)


def portions_of(count, total, reach, skew, full):
    weights = [(1 << 20) // math.isqrt(grade ** skew) + 1 for grade in range(1, count + 1)]
    largest = reach if full else min(reach, max(-(-total // count), total * weights[0] // sum(weights)))
    least = 1 if total - largest >= count - 1 else 0
    holding, rest = [largest] + [least] * (count - 1), total - largest - least * (count - 1)
    while rest > 0:
        free = [i for i in range(1, count) if holding[i] < largest] or [i for i in range(1, count) if holding[i] < reach]
        whole, budget = sum([weights[i] for i in free]), rest
        for i in free:
            more = min(reach - holding[i], max(1, budget * weights[i] // whole), rest)
            holding[i] = holding[i] + more
            rest = rest - more
    return np.array(holding)


def scatter_about(key, shape, spread, limit, pieces=(), kind=jnp.bfloat16):
    drawn = jax.random.normal(key, shape, jnp.float32) * spread
    if len(pieces) > 0:
        drawn = block_scale(key, shape, pieces, -0.22, 0.18) * drawn
    return jnp.clip(drawn, min=-limit, max=limit).astype(kind)


def heavy_noise(key, shape, scale, most, shards, heavy, kind=jnp.bfloat16):
    values = scale * jax.random.normal(key, shape, jnp.float32)
    if shards:
        values = values * block_scale(key, shape, shards, -0.22, 0.18)
    return jnp.clip(raised(values, jax.random.fold_in(key, 3), *heavy), -most, most).astype(kind)


def setup_inputs(seed: int = 0) -> dict:
    splits = jax.random.split(jax.random.key(seed), 8)
    tokens = heavy_noise(splits[0], (MICRO, TOKENS, D), 1.0, 6.0, ((1, 16),), (1, 2, 16, 2.0))
    norm_gain = jnp.clip(1.0 + 0.15 * jax.random.normal(splits[1], (N_SECTION, D), jnp.float32), 0.25, 1.75).astype(jnp.bfloat16)
    router_weight = scatter_about(splits[2], (N_SECTION, D, EXPERTS), D ** -0.5, 0.125, ((0, 2),))
    gate_weight = scatter_about(splits[3], (N_SECTION, EXPERTS, D, FFE), D ** -0.5, 0.125, ((0, 2), (1, 16)))
    up_weight = scatter_about(splits[4], (N_SECTION, EXPERTS, D, FFE), D ** -0.5, 0.125, ((0, 2), (1, 16)))
    down_weight = scatter_about(splits[5], (N_SECTION, EXPERTS, FFE, D), FFE ** -0.5, 0.21875, ((0, 2), (1, 16)))
    routing_keys = jax.random.split(jax.random.fold_in(splits[6], 1), N_SECTION * MICRO * TOKENS // MB_TOK)
    routing_turns = jax.random.permutation(jax.random.fold_in(splits[6], 3), N_SECTION * MICRO * TOKENS // MB_TOK)
    routing = jax.vmap(lambda own, number: deal_out(jax.random.fold_in(splits[6], 2), own, number, MB_TOK, EXPERTS, TOPK, CAP, 1))(routing_keys, routing_turns).reshape((N_SECTION, MICRO, TOKENS, TOPK))
    return dict(tokens=tokens, norm_gain=norm_gain, router_weight=router_weight, gate_weight=gate_weight, up_weight=up_weight, down_weight=down_weight, routing=routing)


EPSILON = 1e-06

def normalize(states, gain):
    values = states.astype(jnp.float32)
    mean_square = lax.optimization_barrier(jnp.mean(values * values, axis=-1, keepdims=True))
    return (values * lax.rsqrt(mean_square + EPSILON) * gain.astype(jnp.float32)).astype(jnp.bfloat16)

def expert_ffn(rows, w_gate, w_up, w_down):
    gated = jnp.dot(rows, w_gate, preferred_element_type=jnp.float32)
    upward = jnp.dot(rows, w_up, preferred_element_type=jnp.float32)
    hidden = (jax.nn.silu(gated) * upward).astype(jnp.bfloat16)
    return jnp.dot(hidden, w_down, preferred_element_type=jnp.float32).astype(jnp.bfloat16)

def routed_hot(routes):
    expert_ids = jnp.arange(EXPERTS, dtype=jnp.int32)
    return (routes[..., None] == expert_ids).astype(jnp.int32).sum(axis=-2)

def layer_block(states, routes, gain, w_router, w_gate, w_up, w_down):
    normed = normalize(states, gain)
    logits = jnp.dot(normed, w_router, preferred_element_type=jnp.float32)
    exps = jnp.exp(logits)
    probs = exps / lax.optimization_barrier(jnp.sum(exps, axis=-1, keepdims=True))
    hot = routed_hot(routes).reshape(N_DP, MB_TOK, EXPERTS)
    rank = jnp.cumsum(hot, axis=1) - hot
    slot_ids = jnp.arange(CAP, dtype=jnp.int32)
    match = ((hot[..., None] == 1) & (rank[..., None] == slot_ids)).astype(jnp.float32)
    blocks = normed.reshape(N_DP, MB_TOK, D).astype(jnp.float32)
    sent = jnp.einsum('jtec,jtd->ejcd', match, blocks).astype(jnp.bfloat16)
    sent = sent.reshape(EXPERTS, N_DP * CAP, D)
    produced = lax.map(lambda item: expert_ffn(item[0], item[1], item[2], item[3]), (sent, w_gate, w_up, w_down))
    produced = lax.optimization_barrier(produced).astype(jnp.float32).reshape(EXPERTS, N_DP, CAP, D)
    chosen = hot.reshape(TOKENS, EXPERTS).astype(jnp.float32) * probs
    weights = (chosen / lax.optimization_barrier(jnp.sum(chosen, axis=-1, keepdims=True))).astype(jnp.bfloat16)
    weights = lax.optimization_barrier(weights).astype(jnp.float32).reshape(N_DP, MB_TOK, EXPERTS)
    combine = match * weights[..., None]
    mixed = jnp.einsum('jtec,ejcd->jtd', combine, produced).reshape(TOKENS, D)
    result = (states.astype(jnp.float32) + mixed).astype(jnp.bfloat16)
    return (result, normed, probs)

def reference(tokens, norm_gain, router_weight, gate_weight, up_weight, down_weight, routing):
    states = tokens
    results = []
    gradients = []
    for layer in range(N_SECTION):

        def run(item):
            return layer_block(item[0], item[1], norm_gain[layer], router_weight[layer], gate_weight[layer], up_weight[layer], down_weight[layer])
        result, normed, probs = lax.map(run, (states, routing[layer]))
        counts = lax.optimization_barrier(jnp.sum(routed_hot(routing[layer]), axis=(0, 1)))
        share = EXPERTS * counts.astype(jnp.float32) / (TOPK * MICRO * TOKENS)
        slope = probs * (share - lax.optimization_barrier(jnp.sum(probs * share, axis=-1, keepdims=True)))
        flat_normed = normed.reshape(MICRO * TOKENS, D).astype(jnp.float32)
        gradient = lax.dot_general(flat_normed, slope.reshape(MICRO * TOKENS, EXPERTS), (((0,), (0,)), ((), ())), precision=lax.Precision.HIGHEST)
        results.append(result)
        gradients.append(gradient)
        states = result
    return (jnp.stack(results), jnp.stack(gradients))
```

```python
import functools

import jax
import jax.numpy as jnp
from jax import lax
from jax.experimental import pallas as pl
from jax.experimental.pallas import tpu as pltpu
from jax.sharding import PartitionSpec as P


EPSILON = 1e-06
LAG = 2


def route_kernel(where_ref, *refs, step, stride, outer, inner, rows, block):
    blocks = refs[:outer]
    gain_ref, router_ref, hot_ref, code_ref = refs[outer : outer + 4]
    outs = refs[outer + 4 :]
    gathered = outs[:inner]
    mixing_ref, normed_ref, probs_ref, weight_ref = outs[inner:]
    gain = gain_ref[...].astype(jnp.float32)
    for k in range(outer):
        values = blocks[k][...].astype(jnp.float32)
        mean_square = jnp.mean(values * values, axis=-1, keepdims=True)
        normed_ref[k * rows : (k + 1) * rows, :] = (
            values * lax.rsqrt(mean_square + EPSILON) * gain
        ).astype(jnp.bfloat16)
    normed = normed_ref[...]
    logits = lax.dot_general(
        router_ref[...], normed, (((1,), (1,)), ((), ())), preferred_element_type=jnp.float32
    )
    exps = jnp.exp(logits)
    probs = exps / jnp.sum(exps, axis=0, keepdims=True)
    probs_ref[...] = probs
    chosen = hot_ref[0] * probs
    weights = (chosen / jnp.sum(chosen, axis=0, keepdims=True)).astype(jnp.bfloat16)
    weight_ref[...] = weights.astype(jnp.float32)
    slot_ids = lax.broadcasted_iota(jnp.int32, (block, normed.shape[0]), 0)
    picks = []
    for j in range(inner):
        expert = where_ref[step * stride + 3 + j]
        match = code_ref[0, pl.ds(expert, 1), :] == slot_ids
        picks.append(jnp.where(match, 1.0, 0.0).astype(jnp.bfloat16))
        mixing_ref[j * block : (j + 1) * block, :] = jnp.where(
            match, weight_ref[pl.ds(expert, 1), :], 0.0
        ).astype(jnp.bfloat16)
    for j in range(inner):
        gathered[j][...] = jnp.dot(
            picks[j], normed, preferred_element_type=jnp.float32
        ).astype(jnp.bfloat16)


def ffn_kernel(*refs, inner, block, tile):
    pieces = refs[:inner]
    gate_ref, up_ref, down_ref = refs[inner : inner + 3]
    outs = refs[inner + 3 : 2 * inner + 3]
    rows_ref, hidden_ref = refs[2 * inner + 3 :]
    for j in range(inner):
        rows_ref[j * block : (j + 1) * block, :] = pieces[j][...]
    rows = rows_ref[...]
    for start in range(0, gate_ref.shape[1], tile):
        part = slice(start, start + tile)
        gated = jnp.dot(rows, gate_ref[:, part], preferred_element_type=jnp.float32)
        upward = jnp.dot(rows, up_ref[:, part], preferred_element_type=jnp.float32)
        hidden_ref[:, part] = (gated * jax.nn.sigmoid(gated) * upward).astype(jnp.bfloat16)
    hidden = hidden_ref[...]
    for start in range(0, down_ref.shape[1], 2 * tile):
        part = slice(start, start + 2 * tile)
        made = jnp.dot(hidden, down_ref[:, part], preferred_element_type=jnp.float32)
        for j in range(inner):
            outs[j][:, part] = made[j * block : (j + 1) * block, :].astype(jnp.bfloat16)


def hot_kernel(where_ref, routing_ref, hot_ref, *, micro, experts):
    chosen_count, _, rows = routing_ref.shape
    ids = lax.broadcasted_iota(jnp.int32, (experts, rows), 0)
    for m in range(micro):
        hot = jnp.zeros((experts, rows), jnp.float32)
        for k in range(chosen_count):
            hot = hot + jnp.where(routing_ref[k, m : m + 1, :] == ids, 1.0, 0.0)
        hot_ref[m * experts : (m + 1) * experts, :] = hot.astype(jnp.bfloat16)


def prepare_kernel(*refs, outer, rows, slots, micro):
    blocks = refs[:outer]
    hot_ref, code_ref, count_ref = refs[outer:]
    column = outer * rows
    token = lax.broadcasted_iota(jnp.int32, (rows, column), 0)
    lane = lax.broadcasted_iota(jnp.int32, (rows, column), 1)
    hot, rank = None, None
    for k in range(outer):
        at = lane - k * rows
        same = jnp.where(at == token, 1.0, 0.0).astype(jnp.bfloat16)
        later = jnp.where((at > token) & (at < rows), 1.0, 0.0).astype(jnp.bfloat16)
        values = blocks[k][...]
        placed = jnp.dot(values, same, preferred_element_type=jnp.float32)
        before = jnp.dot(values, later, preferred_element_type=jnp.float32)
        hot = placed if hot is None else hot + placed
        rank = before if rank is None else rank + before
    plane = lax.broadcasted_iota(jnp.int32, hot.shape, 1) // rows
    hot_ref[...] = hot
    code_ref[...] = jnp.where(hot > 0.5, rank.astype(jnp.int32) + plane * slots, -1)
    sums = jnp.sum(hot, axis=1, keepdims=True)
    experts = count_ref.shape[0]
    count = sums[:experts]
    for m in range(1, micro):
        count = count + sums[m * experts : (m + 1) * experts]
    count_ref[...] = jnp.broadcast_to(count, count_ref.shape)


def mix_kernel(where_ref, *refs, step, stride, outer, inner, rows):
    pieces = refs[:inner]
    mixing_ref, normed_ref, probs_ref, share_ref, grad_in = refs[inner : inner + 5]
    outs = refs[inner + 5 : inner + 5 + outer]
    grad_out = refs[inner + 5 + outer]
    block = pieces[0].shape[0]
    total = None
    for j in range(inner):
        term = lax.dot_general(
            mixing_ref[j * block : (j + 1) * block, :],
            pieces[j][...],
            (((0,), (0,)), ((), ())),
            preferred_element_type=jnp.float32,
        )
        total = term if total is None else total + term
    for k in range(outer):
        outs[k][...] = total[k * rows : (k + 1) * rows, :].astype(outs[k].dtype)
    probs = probs_ref[...]
    normed = normed_ref[...]
    share = share_ref[:, :1]
    slope = probs * (share - jnp.sum(probs * share, axis=0, keepdims=True))
    slope = jnp.where(where_ref[step * stride + 1] > 0, slope, 0.0)
    high = slope.astype(jnp.bfloat16)
    rest = slope - high.astype(jnp.float32)
    middle = rest.astype(jnp.bfloat16)
    low = (rest - middle.astype(jnp.float32)).astype(jnp.bfloat16)
    total = grad_in[...]
    for term in (high, middle, low):
        total = total + jnp.dot(term, normed, preferred_element_type=jnp.float32)
    grad_out[...] = total


def total_kernel(where_ref, *refs, step, stride, outer, earlier, entering):
    own_ref, mixed_ref = refs[:2]
    arrived = refs[2 : outer + 1]
    older = refs[outer + 1 : outer + 1 + earlier]
    rest = refs[outer + 1 + earlier :]
    position = where_ref[step * stride + 2]
    total = own_ref[...].astype(jnp.float32) + mixed_ref[...]
    for ref in arrived:
        total = total + ref[...].astype(jnp.float32)
    result = total.astype(jnp.bfloat16)
    if entering:
        entering_ref, payload_ref = rest[0], rest[-1]
        payload_ref[...] = jnp.where(position == entering - 1, entering_ref[...], result)
        rest = rest[1:-1]
    rest[0][...] = result
    if earlier:
        chosen = result
        for s, ref in enumerate(older):
            chosen = jnp.where(position == s, ref[...], chosen)
        rest[1][...] = chosen


def split_kernel(where_ref, grad_ref, *outs, replicas):
    share_rows = grad_ref.shape[1] // replicas
    for j, out in enumerate(outs):
        expert = where_ref[3 + j]
        piece = jnp.zeros((grad_ref.shape[0], share_rows), jnp.float32)
        for n in range(replicas):
            part = grad_ref[:, n * share_rows : (n + 1) * share_rows]
            piece = jnp.where(expert == n, part, piece)
        out[...] = piece.astype(jnp.bfloat16)


def whole(shape):
    return pl.BlockSpec(shape, lambda *_: (0,) * len(shape))


def few(sections):
    return sections <= 2


def plane_size(count):
    inner = 1
    while inner * inner < count or count % inner:
        inner += 1
    return inner


def on_device(tokens, norm_gain, router_weight, gate_weight, up_weight, down_weight, routing):
    sections = lax.axis_size("section")
    replicas = lax.axis_size("dp")
    position = lax.axis_index("section")
    place = lax.axis_index("dp")
    inner = plane_size(replicas)
    outer = replicas // inner
    plane, seat = place // inner, place % inner
    micro, rows, width = tokens.shape
    experts = router_weight.shape[2]
    chosen_count = routing.shape[3]
    slots = min(rows, rows * chosen_count // experts + 1)
    block = -(-outer * slots // 8) * 8
    total_rows = micro * rows * replicas
    column = outer * rows
    w_router = router_weight[0]
    w_gate = gate_weight[0, 0]
    w_up = up_weight[0, 0]
    w_down = down_weight[0, 0]
    axes = ("section", "dp")
    everyone = [(s, o, i) for s in range(sections) for o in range(outer) for i in range(inner)]

    def flat(s, o, i):
        return ((s % sections) * outer + o % outer) * inner + i % inner

    def send(value, ds, do, di):
        pairs = [(flat(s, o, i), flat(s + ds, o + do, i + di)) for s, o, i in everyone]
        return lax.ppermute(value, axes, pairs)

    unrolled = few(sections)
    lag = LAG if unrolled else 1
    steps = micro + lag * (sections - 1)
    moment = jnp.arange(steps, dtype=jnp.int32)[:, None] - lag * position
    where = jnp.concatenate(
        [
            jnp.clip(moment, 0, micro - 1),
            ((moment >= 0) & (moment < micro)).astype(jnp.int32),
            jnp.broadcast_to(position, (steps, 1)),
            jnp.broadcast_to(
                (plane * inner + (seat + jnp.arange(inner, dtype=jnp.int32)) % inner)[None, :],
                (steps, inner),
            ),
        ],
        axis=1,
    ).astype(jnp.int32)
    stride = where.shape[1]
    where = where.reshape(-1)
    hot_own = pl.pallas_call(
        functools.partial(hot_kernel, micro=micro, experts=experts),
        grid_spec=pltpu.PrefetchScalarGridSpec(
            num_scalar_prefetch=1,
            grid=(1,),
            in_specs=[whole((chosen_count, micro, rows))],
            out_specs=whole((micro * experts, rows)),
        ),
        out_shape=jax.ShapeDtypeStruct((micro * experts, rows), jnp.bfloat16),
        compiler_params=pltpu.CompilerParams(vmem_limit_bytes=4 << 20),
        name="hot",
    )(where, routing[0].transpose(2, 0, 1))
    hot_blocks = [hot_own] + [send(hot_own, 0, k, 0) for k in range(1, outer)]
    unused = position < 0
    w_gate, w_up, w_down = [
        jnp.where(unused, jnp.zeros_like(value), value) for value in (w_gate, w_up, w_down)
    ]
    hot_all, codes, counts = pl.pallas_call(
        functools.partial(prepare_kernel, outer=outer, rows=rows, slots=slots, micro=micro),
        grid=(1,),
        in_specs=[whole((micro * experts, rows))] * outer,
        out_specs=[whole((micro * experts, column))] * 2 + [whole((experts, 128))],
        out_shape=[
            jax.ShapeDtypeStruct((micro * experts, column), jnp.float32),
            jax.ShapeDtypeStruct((micro * experts, column), jnp.int32),
            jax.ShapeDtypeStruct((experts, 128), jnp.float32),
        ],
        compiler_params=pltpu.CompilerParams(vmem_limit_bytes=4 << 20),
        name="prepare",
    )(*hot_blocks)
    hot_all = hot_all.reshape(micro, experts, column)
    codes = codes.reshape(micro, experts, column)
    counts = counts + sum(send(counts, 0, 0, j) for j in range(1, inner))
    share = experts * counts / (chosen_count * total_rows)
    router_rows = w_router.T
    gain_row = norm_gain

    def stage_route(where, step, blocks):
        table = pl.BlockSpec((1, experts, column), lambda g, where: (where[step * stride], 0, 0))
        outs = pl.pallas_call(
            functools.partial(
                route_kernel,
                step=step,
                stride=stride,
                outer=outer,
                inner=inner,
                rows=rows,
                block=block,
            ),
            grid_spec=pltpu.PrefetchScalarGridSpec(
                num_scalar_prefetch=1,
                grid=(1,),
                in_specs=[whole((rows, width))] * outer
                + [whole((1, width)), whole((experts, width)), table, table],
                out_specs=[whole((block, width))] * inner
                + [
                    whole((inner * block, column)),
                    whole((column, width)),
                    whole((experts, column)),
                ],
                scratch_shapes=[pltpu.VMEM((experts, column), jnp.float32)],
            ),
            out_shape=[jax.ShapeDtypeStruct((block, width), jnp.bfloat16)] * inner
            + [
                jax.ShapeDtypeStruct((inner * block, column), jnp.bfloat16),
                jax.ShapeDtypeStruct((column, width), jnp.bfloat16),
                jax.ShapeDtypeStruct((experts, column), jnp.float32),
            ],
            cost_estimate=pl.CostEstimate(
                flops=2 * inner * block * column * width, bytes_accessed=3 << 20, transcendentals=0
            ),
            compiler_params=pltpu.CompilerParams(vmem_limit_bytes=12 << 20),
            name="route",
        )(where, *blocks, gain_row, router_rows, hot_all, codes)
        return outs[:inner], outs[inner], outs[inner + 1], outs[inner + 2]

    hidden_width = w_gate.shape[1]
    tile = 256 if hidden_width % 256 == 0 else hidden_width

    def stage_ffn(pieces):
        return pl.pallas_call(
            functools.partial(ffn_kernel, inner=inner, block=block, tile=tile),
            grid=(1,),
            in_specs=[whole((block, width))] * inner
            + [whole((width, hidden_width))] * 2
            + [whole((hidden_width, width))],
            out_specs=[whole((block, width))] * inner,
            out_shape=[jax.ShapeDtypeStruct((block, width), jnp.bfloat16)] * inner,
            scratch_shapes=[
                pltpu.VMEM((inner * block, width), jnp.bfloat16),
                pltpu.VMEM((inner * block, hidden_width), jnp.bfloat16),
            ],
            cost_estimate=pl.CostEstimate(
                flops=6 * inner * block * width * hidden_width,
                bytes_accessed=6 * width * hidden_width,
                transcendentals=inner * block * hidden_width,
            ),
            compiler_params=pltpu.CompilerParams(vmem_limit_bytes=28 << 20),
            name="ffn",
        )(*pieces, w_gate, w_up, w_down)

    def stage_mix(where, step, pieces, mixing, normed, probs, gradient):
        outs = pl.pallas_call(
            functools.partial(
                mix_kernel, step=step, stride=stride, outer=outer, inner=inner, rows=rows
            ),
            grid_spec=pltpu.PrefetchScalarGridSpec(
                num_scalar_prefetch=1,
                grid=(1,),
                in_specs=[whole((block, width))] * inner
                + [whole((inner * block, column)), whole((column, width))]
                + [whole((experts, column)), whole((experts, 128)), whole((experts, width))],
                out_specs=[whole((rows, width))] * outer + [whole((experts, width))],
            ),
            out_shape=[
                jax.ShapeDtypeStruct((rows, width), jnp.bfloat16 if k else jnp.float32)
                for k in range(outer)
            ]
            + [jax.ShapeDtypeStruct((experts, width), jnp.float32)],
            cost_estimate=pl.CostEstimate(
                flops=2 * inner * block * column * width, bytes_accessed=2 << 20, transcendentals=0
            ),
            compiler_params=pltpu.CompilerParams(vmem_limit_bytes=12 << 20),
            name="mix",
        )(where, *pieces, mixing, normed, probs, share, gradient)
        return outs[:outer], outs[outer]

    def stage_total(where, step, own, mixed, arrived, older, entering):
        count = 1 + bool(older) + (entering is not None)
        inputs = [own, mixed, *arrived, *older] + ([] if entering is None else [entering])
        return pl.pallas_call(
            functools.partial(
                total_kernel,
                step=step,
                stride=stride,
                outer=outer,
                earlier=len(older),
                entering=0 if entering is None else sections,
            ),
            grid_spec=pltpu.PrefetchScalarGridSpec(
                num_scalar_prefetch=1,
                grid=(1,),
                in_specs=[whole((rows, width))] * len(inputs),
                out_specs=[whole((rows, width))] * count,
            ),
            out_shape=[jax.ShapeDtypeStruct((rows, width), jnp.bfloat16)] * count,
            cost_estimate=pl.CostEstimate(
                flops=64 * rows * width, bytes_accessed=20 * rows * width, transcendentals=0
            ),
            compiler_params=pltpu.CompilerParams(vmem_limit_bytes=8 << 20),
            name="total",
        )(where, *inputs)

    def advance(where, step, payload, entering, older, gradient):
        blocks = [send(payload, 1, k, 0) for k in range(outer)]
        gathered, mixing, normed, probs = stage_route(where, step, blocks)
        pieces = [gathered[0]] + [send(gathered[j], 0, 0, j) for j in range(1, inner)]
        produced = stage_ffn(pieces)
        pieces = [produced[0]] + [send(produced[j], 0, 0, -j) for j in range(1, inner)]
        mixed, gradient = stage_mix(
            where, step, pieces, mixing, normed, probs, gradient
        )
        arrived = [send(mixed[k], 0, -k, 0) for k in range(1, outer)]
        outs = stage_total(where, step, blocks[0], mixed[0], arrived, older, entering)
        return outs, gradient

    gradient = jnp.zeros((experts, width), jnp.float32)
    if unrolled:
        results, kept = [], []
        payloads = [tokens[min(step, micro - 1)] for step in range(lag)]
        for step in range(steps):
            entering = tokens[min(step + lag, micro - 1)] if step + lag < steps else None
            first = step - lag * (sections - 1)
            older = [results[first + lag * s] for s in range(sections - 1)] if first >= 0 else []
            outs, gradient = advance(where, step, payloads[step], entering, older, gradient)
            results.append(outs[0])
            if entering is not None:
                payloads.append(outs[-1])
            if first >= 0:
                kept.append(outs[1] if older else outs[0])
        outputs = jnp.stack(kept)
    else:

        def body(step, carry):
            payload, gradient, outputs = carry
            row = lax.dynamic_index_in_dim(where.reshape(steps, stride), step, 0, keepdims=False)
            entering = lax.dynamic_index_in_dim(
                tokens, jnp.minimum(step + lag, micro - 1), 0, keepdims=False
            )
            outs, gradient = advance(row, 0, payload, entering, [], gradient)
            result, payload = outs
            previous = lax.dynamic_index_in_dim(outputs, row[0], 0, keepdims=False)
            result = jnp.where(row[1] > 0, result, previous)
            outputs = lax.dynamic_update_index_in_dim(outputs, result, row[0], 0)
            return payload, gradient, outputs

        outputs = jnp.zeros((micro, rows, width), jnp.bfloat16)
        _, gradient, outputs = lax.fori_loop(0, steps, body, (tokens[0], gradient, outputs))
    share_rows = width // replicas
    pieces = pl.pallas_call(
        functools.partial(split_kernel, replicas=replicas),
        grid_spec=pltpu.PrefetchScalarGridSpec(
            num_scalar_prefetch=1,
            grid=(1,),
            in_specs=[whole((experts, width))],
            out_specs=[whole((experts, share_rows))] * inner,
        ),
        out_shape=[jax.ShapeDtypeStruct((experts, share_rows), jnp.bfloat16)] * inner,
        compiler_params=pltpu.CompilerParams(vmem_limit_bytes=4 << 20),
        name="split",
    )(where, gradient)
    grad_rows = pieces[0].astype(jnp.float32)
    for j in range(1, inner):
        grad_rows = grad_rows + send(pieces[j], 0, 0, j).astype(jnp.float32)
    grad_rows = grad_rows.T
    return (outputs[None], grad_rows[None])


def solution(mesh):
    placed = (
        P(None, "dp", None),
        P("section", None),
        P("section", None, None),
        P("section", "dp", None, None),
        P("section", "dp", None, None),
        P("section", "dp", None, None),
        P("section", None, "dp", None),
    )
    return jax.shard_map(
        on_device,
        mesh=mesh,
        in_specs=placed,
        out_specs=(P("section", None, "dp", None), P("section", "dp", None)),
        check_vma=False,
    )
```
